32 devices in a mesh: mem: 4 (over z), hor: 2 (over x), grp: 4 (over y, core).
Axes of the slice: x: 2, y: 2, z: 4, core: 2. Of those that a mesh axis runs over, the one named last changes fastest.
Arguments:
- ensemble: float32 [128, 2, 32, 1024], P(('mem', 'grp'), None, None, 'hor'), may hold values from -1 to 1
- coupling: float32 [32, 32], replicated, may hold values from -1 to 1
- obs_column: int32 [2, 16, 2, 512], P(None, ('mem', 'grp'), 'hor'), may hold values from 0 to 511
- obs_level: int32 [2, 16, 2, 512], P(None, ('mem', 'grp'), 'hor'), may hold values from 0 to 1
- obs_value: float32 [2, 16, 2, 512], P(None, ('mem', 'grp'), 'hor'), may hold values from -6 to 6
- obs_error: float32 [2, 16, 2, 512], P(None, ('mem', 'grp'), 'hor'), may hold values from 0.25 to 4
- obs_live: int32 [2, 16, 2, 512], P(None, ('mem', 'grp'), 'hor'), may hold values 0 or 1
- partners: int32 [16, 2, 2], P(('mem', 'grp'), 'hor'), may hold values from 0 to 15, as said below
Outputs:
- analysed: float32 [128, 2, 32, 1024], P(('mem', 'grp'), None, None, 'hor')
The draws below stay inside these ranges and needn't reach their ends.
Inputs may be any that keep to these rules, and one draw needn't show every extreme that they name: `partners`: each row holds 2 different slab numbers, none of them the row's own slab.
All inputs are finite; a program needn't handle non-finite values. No bound on the sum of `obs_live` on one device may be relied on, other than what follows from the above.
Results may differ from the reference program's by a relative error of at most 0.0003.
Values sent between devices are 32-bit elements; how exact they have to be, the bound alone decides.
A program may use at most 64 MiB of HBM per device.

```python
import math
import jax
import jax.numpy as jnp
from jax import lax

MEMBERS = 128
LEVELS = 32
COL_DEV = 512
OBS_SLOTS = 512
SUBSTEPS = 4
CYCLES = 2
ROOT_STEPS = 8
PARTNER_COUNT = 2
SLABS = 16
TILES = 2
SLAB_LEVELS = 2
COLUMNS = 1024


def draw_partners(key, part):
    first_key, second_key = jax.random.split(jax.random.fold_in(key, 7))
    first = jax.random.randint(first_key, (SLABS, TILES), 1, SLABS)
    second = jax.random.randint(second_key, (SLABS, TILES), 1, SLABS - 1)
    second = second + (second >= first).astype(jnp.int32)
    own_slab = jnp.arange(SLABS, dtype=jnp.int32)[:, None]
    chosen = jnp.stack([(own_slab + first) % SLABS, (own_slab + second) % SLABS], axis=-1)
    return chosen.astype(jnp.int32)


def place_ends(drawn, own_key, smallest, top_value):
    spot = [jax.random.randint(jax.random.fold_in(own_key, axis), (), 0, length) for axis, length in enumerate(drawn.shape)]
    main_axis = drawn.shape.index(max(drawn.shape))
    neighbour = spot[:main_axis] + [(spot[main_axis] + 1) % drawn.shape[main_axis]] + spot[main_axis + 1:]
    return drawn.at[tuple(spot)].set(smallest).at[tuple(neighbour)].set(top_value)


def block_levels(key, extent, cuts, least, top_value):
    gain = 1.0
    for axis_at, shards_of in cuts:
        draws = jax.random.uniform(jax.random.fold_in(jax.random.fold_in(key, 6), axis_at), (shards_of,), jnp.float32, least / len(cuts), top_value / len(cuts))
        gain = gain * jnp.repeat(jnp.exp(draws), extent[axis_at] // shards_of).reshape((-1,) + (1,) * (len(extent) - 1 - axis_at))
    return gain


def gaussian(stream_key, dims, scale, bound, pieces=(), held_as=jnp.bfloat16):
    array = jax.random.normal(stream_key, dims, jnp.float32) * scale
    if len(pieces) > 0:
        array = block_levels(stream_key, dims, pieces, -0.22, 0.18) * array
    return jnp.clip(array, min=-bound, max=bound).astype(held_as)


def setup_inputs(seed: int = 0) -> dict:
    streams_of = jax.random.split(jax.random.key(seed), 9)
    ensemble = gaussian(streams_of[0], (MEMBERS, 2, LEVELS, COLUMNS), 0.25, 1.0, ((0, 16), (3, 2)), jnp.float32)
    coupling = gaussian(streams_of[1], (LEVELS, LEVELS), LEVELS ** -0.5, 1.0, (), jnp.float32)
    obs_column = place_ends(jax.random.randint(streams_of[2], (CYCLES, SLABS, TILES, OBS_SLOTS), 0, COL_DEV), jax.random.fold_in(streams_of[2], 1), 0, COL_DEV - 1).astype(jnp.int32)
    obs_level = place_ends(jax.random.randint(streams_of[3], (CYCLES, SLABS, TILES, OBS_SLOTS), 0, SLAB_LEVELS), jax.random.fold_in(streams_of[3], 1), 0, SLAB_LEVELS - 1).astype(jnp.int32)
    obs_value = gaussian(streams_of[4], (CYCLES, SLABS, TILES, OBS_SLOTS), 1.0, 6.0, ((1, 16), (2, 2)), jnp.float32)
    obs_error = jnp.clip(jnp.exp(math.log(4.0) - 2.7725887 * jax.random.uniform(streams_of[5], (CYCLES, SLABS, TILES, OBS_SLOTS), jnp.float32) ** block_levels(streams_of[5], (CYCLES, SLABS, TILES, OBS_SLOTS), ((1, 16), (2, 2)), -0.2, 0.2)), 0.25, 4.0)
    obs_live = place_ends((jax.random.randint(streams_of[6], (CYCLES, SLABS, TILES, OBS_SLOTS), 0, 4) < 3).astype(jnp.int32), jax.random.fold_in(streams_of[6], 1), 0, 1)
    partners = draw_partners(jax.random.fold_in(streams_of[8], 71), 0)
    return {"ensemble": ensemble, "coupling": coupling, "obs_column": obs_column, "obs_level": obs_level, "obs_value": obs_value, "obs_error": obs_error, "obs_live": obs_live, "partners": partners}


time_step = 0.2

def centred(field):
    return (jnp.roll(field, -1, axis=-1) - jnp.roll(field, 1, axis=-1)) * 0.5

def substep(velocity, height, coupling):
    pressure = jnp.einsum('lk,mkc->mlc', coupling, height, precision=lax.Precision.HIGHEST)
    moved = velocity - time_step * (velocity * centred(velocity) + centred(pressure))
    fluxes = moved * height
    height_new = height - time_step * centred(fluxes)
    return (moved, height_new)

def observe(patch, column, level, value, error, live):
    width = patch.shape[0]
    cells = patch.shape[-1]
    heights = patch[:, 1].reshape(width, -1)
    position = (level * cells + column).astype(jnp.int32)
    observed = jnp.take(heights, position, axis=1)
    average = lax.optimization_barrier(jnp.mean(observed, axis=0))
    anomalies = observed - average
    weight = live.astype(jnp.float32) / error
    gram_matrix = jnp.dot(anomalies * weight, anomalies.T, precision=lax.Precision.HIGHEST)
    innovation = jnp.dot(anomalies, weight * (value - average), precision=lax.Precision.HIGHEST)
    return (gram_matrix, innovation)

def analyse(patch, gram_sum, vector_sum, count):
    width = patch.shape[0]
    identity = jnp.eye(width, dtype=jnp.float32)
    blended = (width - 1.0) * identity + gram_sum / (count + 1.0)
    bvector = vector_sum / (count + 1.0)
    frobenius = jnp.sqrt(jnp.sum(blended * blended))
    iterate = blended / frobenius
    inverse_root = identity
    for step_index in range(ROOT_STEPS):
        newton = 1.5 * identity - 0.5 * jnp.dot(inverse_root, iterate, precision=lax.Precision.HIGHEST)
        iterate = jnp.dot(iterate, newton, precision=lax.Precision.HIGHEST)
        inverse_root = jnp.dot(newton, inverse_root, precision=lax.Precision.HIGHEST)
    spread = inverse_root * (jnp.sqrt(width - 1.0) / jnp.sqrt(frobenius))
    inner = jnp.dot(inverse_root, bvector, precision=lax.Precision.HIGHEST)
    mean_weight = jnp.dot(inverse_root, inner, precision=lax.Precision.HIGHEST) / frobenius
    transform = mean_weight[:, None] + spread
    flat = patch.reshape(width, -1)
    average = lax.optimization_barrier(jnp.mean(flat, axis=0))
    anomalies = flat - average
    result = average + jnp.dot(transform.T, anomalies, precision=lax.Precision.HIGHEST)
    return result.reshape(patch.shape)

def reference(ensemble, coupling, obs_column, obs_level, obs_value, obs_error, obs_live, partners):
    members = ensemble
    tile_index = jnp.arange(TILES, dtype=jnp.int32)[None, :]
    for cycle_index in range(CYCLES):
        velocity, height = (members[:, 0], members[:, 1])
        for step_index in range(SUBSTEPS):
            velocity, height = substep(velocity, height, coupling)
        members = jnp.stack([velocity, height], axis=1)
        patches = members.reshape(MEMBERS, 2, SLABS, SLAB_LEVELS, TILES, COL_DEV).transpose(2, 4, 0, 1, 3, 5)
        flat_patches = patches.reshape(SLABS * TILES, MEMBERS, 2, SLAB_LEVELS, COL_DEV)

        def observe_one(items):
            return observe(items[0], items[1], items[2], items[3], items[4], items[5])
        grams, vectors = lax.map(observe_one, (flat_patches, obs_column[cycle_index].reshape(-1, OBS_SLOTS), obs_level[cycle_index].reshape(-1, OBS_SLOTS), obs_value[cycle_index].reshape(-1, OBS_SLOTS), obs_error[cycle_index].reshape(-1, OBS_SLOTS), obs_live[cycle_index].reshape(-1, OBS_SLOTS)))
        grams = grams.reshape(SLABS, TILES, MEMBERS, MEMBERS)
        vectors = vectors.reshape(SLABS, TILES, MEMBERS)
        gram_sum = grams
        vector_sum = vectors
        for which in range(PARTNER_COUNT):
            gram_sum = gram_sum + grams[partners[:, :, which], tile_index]
            vector_sum = vector_sum + vectors[partners[:, :, which], tile_index]

        def analyse_one(items):
            return analyse(items[0], items[1], items[2], PARTNER_COUNT)
        updated = lax.map(analyse_one, (flat_patches, gram_sum.reshape(-1, MEMBERS, MEMBERS), vector_sum.reshape(-1, MEMBERS)))
        members = updated.reshape(SLABS, TILES, MEMBERS, 2, SLAB_LEVELS, COL_DEV).transpose(2, 3, 0, 4, 1, 5).reshape(MEMBERS, 2, LEVELS, COLUMNS)
    return members
```

```python
import functools

import jax
import jax.numpy as jnp
from jax import lax
from jax.experimental import pallas as pl
from jax.experimental.pallas import tpu as pltpu
from jax.sharding import PartitionSpec as P

SUBSTEPS = 4
ROOT_STEPS = 8
MESH = pl.DeviceIdType.MESH


time_step = 0.2


def sent(piece, axis, pairs):
    width = piece.shape[-1]
    packed = jnp.moveaxis(piece, -1, 0).reshape(width, -1)
    moved = lax.ppermute(packed, axis, pairs)
    return jnp.moveaxis(moved.reshape((width,) + piece.shape[:-1]), 0, -1)


def with_halo(block, axis, width):
    count = lax.axis_size(axis)
    forward = [(i, (i + 1) % count) for i in range(count)]
    backward = [(target, source) for source, target in forward]
    low = sent(block[..., block.shape[-1] - width :], axis, forward)
    high = sent(block[..., :width], axis, backward)
    return jnp.concatenate([low, block, high], axis=-1)


def centred(field):
    return (field[..., 2:] - field[..., :-2]) * 0.5


def substep(velocity, height, coupling):
    pressure = jnp.einsum("lk,mkc->mlc", coupling, height, precision=lax.Precision.HIGHEST)
    inner = velocity[..., 1:-1]
    moved = inner - time_step * (inner * centred(velocity) + centred(pressure))
    fluxes = moved * height[..., 1:-1]
    height_new = height[..., 2:-2] - time_step * centred(fluxes)
    return (moved[..., 1:-1], height_new)


def advance(members, coupling):
    extended = with_halo(members, "hor", 2 * SUBSTEPS)
    velocity, height = (extended[:, 0], extended[:, 1])
    for step_index in range(SUBSTEPS):
        velocity, height = substep(velocity, height, coupling)
    members = jnp.stack([velocity, height], axis=1)
    return members


def to_patches(members, mem_count, grp_count):
    block, fields, levels, cells = members.shape
    slab_count = mem_count * grp_count
    thin = levels // slab_count
    shaped = members.reshape(1, block, fields, slab_count, thin, cells)
    moved = lax.all_to_all(shaped, ("mem", "grp"), split_axis=3, concat_axis=0, tiled=True)
    return moved.reshape(slab_count * block, fields, thin, cells)


def from_patches(patch, mem_count, grp_count):
    width, fields, thin, cells = patch.shape
    slab_count = mem_count * grp_count
    block = width // slab_count
    shaped = patch.reshape(slab_count, block, fields, 1, thin, cells)
    moved = lax.all_to_all(shaped, ("mem", "grp"), split_axis=0, concat_axis=3, tiled=True)
    return moved.reshape(block, fields, slab_count * thin, cells)


def split(value):
    high = value.astype(jnp.bfloat16)
    return high, (value - high.astype(jnp.float32)).astype(jnp.bfloat16)


def product(left, right, across=0):
    dims = (((1,), (across,)), ((), ()))

    def one(a, b):
        return lax.dot_general(a, b, dims, preferred_element_type=jnp.float32)

    left_high, left_low = split(left)
    right_high, right_low = split(right)
    return one(left_high, right_high) + (one(left_high, right_low) + one(left_low, right_high))


def analysis(
    sizes, count,
    seen_ref, value_ref, error_ref, live_ref, blend_ref, flat_ref, out_ref,
    own, column, partial, arrived, peers_blend,
    send_a, recv_a, send_b, recv_b, send_c, recv_c,
):
    mem_count, grp_count = sizes
    mem = lax.axis_index("mem")
    grp = lax.axis_index("grp")

    def mem_peer(step):
        return lax.rem(mem + step, mem_count)

    def grp_peer(step):
        return lax.rem(grp + step, grp_count)

    barrier = pltpu.get_barrier_semaphore()
    for step in range(1, mem_count):
        pl.semaphore_signal(barrier, inc=1, device_id={"mem": mem_peer(step)}, device_id_type=MESH)
    for step in range(1, grp_count):
        pl.semaphore_signal(barrier, inc=1, device_id={"grp": grp_peer(step)}, device_id_type=MESH)

    width = seen_ref.shape[0]
    seen = seen_ref[...]
    average = jnp.mean(seen, axis=0, keepdims=True)
    anomalies = seen - average
    weight = live_ref[...].astype(jnp.float32) / error_ref[...]
    pull = weight * (value_ref[...] - average)
    rows = jnp.concatenate(
        [anomalies * weight, jnp.broadcast_to(pull, (8, pull.shape[1]))], axis=0
    )
    own[...] = product(rows, anomalies, 1)

    pl.semaphore_wait(barrier, mem_count + grp_count - 2)
    blends = []
    for step in range(1, grp_count):
        copy = pltpu.make_async_remote_copy(
            src_ref=blend_ref, dst_ref=peers_blend.at[step - 1],
            send_sem=send_b.at[step - 1], recv_sem=recv_b.at[step - 1],
            device_id={"grp": grp_peer(step)}, device_id_type=MESH,
        )
        copy.start()
        blends.append(copy)
    gathers = []
    for step in range(1, mem_count):
        copy = pltpu.make_async_remote_copy(
            src_ref=own, dst_ref=column.at[step - 1],
            send_sem=send_a.at[step - 1], recv_sem=recv_a.at[step - 1],
            device_id={"mem": mem_peer(step)}, device_id_type=MESH,
        )
        copy.start()
        gathers.append(copy)
    for copy in blends:
        copy.wait()
    lanes = lax.broadcasted_iota(jnp.int32, (1, blend_ref.shape[1]), 1)

    def share(row, step):
        place = lax.rem(mem + mem_count - step, mem_count) * grp_count + grp
        return jnp.sum(jnp.where(lanes == place, row[0:1], 0.0), axis=1, keepdims=True)

    for copy in gathers:
        copy.wait()

    def blended_for(row):
        total = share(row, 0) * own[...]
        for step in range(1, mem_count):
            total = total + share(row, step) * column[step - 1]
        return total

    returns = []
    for step in range(1, grp_count):
        partial[step - 1] = blended_for(peers_blend[step - 1])
        copy = pltpu.make_async_remote_copy(
            src_ref=partial.at[step - 1], dst_ref=arrived.at[step - 1],
            send_sem=send_c.at[step - 1], recv_sem=recv_c.at[step - 1],
            device_id={"grp": grp_peer(grp_count - step)}, device_id_type=MESH,
        )
        copy.start()
        returns.append(copy)
    total = blended_for(blend_ref[...])
    flat = flat_ref[...]
    flat_average = jnp.mean(flat, axis=0, keepdims=True)
    for copy in returns:
        copy.wait()
    for step in range(1, grp_count):
        total = total + arrived[step - 1]

    total = total / (count + 1.0)
    square = (width, width)
    identity = (
        lax.broadcasted_iota(jnp.int32, square, 0) == lax.broadcasted_iota(jnp.int32, square, 1)
    ).astype(jnp.float32)
    blended = (width - 1.0) * identity + total[:width]
    bvector = total[width:]
    squares = jnp.sum(jnp.sum(blended * blended, axis=1, keepdims=True), axis=0, keepdims=True)
    frobenius = jnp.sqrt(squares)
    iterate = blended / frobenius
    newton = 1.5 * identity - 0.5 * iterate
    inverse_root = newton
    for step in range(1, ROOT_STEPS):
        iterate = product(newton, iterate)
        newton = 1.5 * identity - 0.5 * product(inverse_root, iterate)
        inverse_root = product(newton, inverse_root)
    spread = inverse_root * (jnp.sqrt(width - 1.0) / jnp.sqrt(frobenius))
    inner = product(bvector, inverse_root)
    mean_weight = product(inner, inverse_root) / frobenius
    transposed = spread + mean_weight[0:1]
    out_ref[...] = flat_average + product(transposed, flat - flat_average)


def analysed(sizes, count, seen, value, error, live, blend, flat):
    width = seen.shape[0]
    mem_count, grp_count = sizes
    tall = (width + 8, width)
    vmem = pl.BlockSpec(memory_space=pltpu.VMEM)
    dma = pltpu.SemaphoreType.DMA
    return pl.pallas_call(
        functools.partial(analysis, sizes, count),
        out_shape=jax.ShapeDtypeStruct(flat.shape, jnp.float32),
        in_specs=[vmem] * 6,
        out_specs=vmem,
        scratch_shapes=[
            pltpu.VMEM(tall, jnp.float32),
            pltpu.VMEM((mem_count - 1,) + tall, jnp.float32),
            pltpu.VMEM((grp_count - 1,) + tall, jnp.float32),
            pltpu.VMEM((grp_count - 1,) + tall, jnp.float32),
            pltpu.VMEM((grp_count - 1,) + blend.shape, jnp.float32),
            dma((mem_count - 1,)), dma((mem_count - 1,)),
            dma((grp_count - 1,)), dma((grp_count - 1,)),
            dma((grp_count - 1,)), dma((grp_count - 1,)),
        ],
        compiler_params=pltpu.CompilerParams(collective_id=0, has_side_effects=True),
    )(seen, value[None], error[None], live[None], blend, flat)


def shards(ensemble, coupling, obs_column, obs_level, obs_value, obs_error, obs_live, partners):
    mem_count = lax.axis_size("mem")
    grp_count = lax.axis_size("grp")
    slab_count = mem_count * grp_count
    own_slab = lax.axis_index("mem") * grp_count + lax.axis_index("grp")
    lanes = max(128, -(-slab_count // 128) * 128)
    slab_numbers = jnp.arange(lanes, dtype=jnp.int32)
    chosen = partners[0, 0]
    count = chosen.shape[0]
    blend_weights = (slab_numbers == own_slab).astype(jnp.float32)
    blend_weights = blend_weights + jnp.sum(
        (slab_numbers[:, None] == chosen[None, :]).astype(jnp.float32), axis=1
    )
    blend = jnp.broadcast_to(blend_weights, (8, lanes))
    width = ensemble.shape[0] * slab_count
    cells = ensemble.shape[3]
    members = ensemble
    for cycle_index in range(obs_column.shape[0]):
        members = advance(members, coupling)
        patch = to_patches(members, mem_count, grp_count)
        place = obs_level[cycle_index, 0, 0] * cells + obs_column[cycle_index, 0, 0]
        observed = jnp.take(patch[:, 1].reshape(width, -1), place, axis=1)
        flat = analysed(
            (mem_count, grp_count), count, observed,
            obs_value[cycle_index, 0, 0], obs_error[cycle_index, 0, 0],
            obs_live[cycle_index, 0, 0], blend, patch.reshape(width, -1),
        )
        members = from_patches(flat.reshape(patch.shape), mem_count, grp_count)
    return members


def solution(mesh):
    in_specs = (
        P(("mem", "grp"), None, None, "hor"),
        P(),
        P(None, ("mem", "grp"), "hor", None),
        P(None, ("mem", "grp"), "hor", None),
        P(None, ("mem", "grp"), "hor", None),
        P(None, ("mem", "grp"), "hor", None),
        P(None, ("mem", "grp"), "hor", None),
        P(("mem", "grp"), "hor", None),
    )
    out_specs = P(("mem", "grp"), None, None, "hor")
    return jax.shard_map(shards, mesh=mesh, in_specs=in_specs, out_specs=out_specs, check_vma=False)
```

```python
import functools

import jax
import jax.numpy as jnp
from jax import lax
from jax.experimental import pallas as pl
from jax.experimental.pallas import tpu as pltpu
from jax.sharding import PartitionSpec as P

SUBSTEPS = 4
ROOT_STEPS = 8
MESH = pl.DeviceIdType.MESH


time_step = 0.2


def sent(piece, axis, pairs):
    width = piece.shape[-1]
    packed = jnp.moveaxis(piece, -1, 0).reshape(width, -1)
    moved = lax.ppermute(packed, axis, pairs)
    return jnp.moveaxis(moved.reshape((width,) + piece.shape[:-1]), 0, -1)


def with_halo(block, axis, width):
    count = lax.axis_size(axis)
    forward = [(i, (i + 1) % count) for i in range(count)]
    backward = [(target, source) for source, target in forward]
    low = sent(block[..., block.shape[-1] - width :], axis, forward)
    high = sent(block[..., :width], axis, backward)
    return jnp.concatenate([low, block, high], axis=-1)


def centred(field):
    return (field[..., 2:] - field[..., :-2]) * 0.5


def substep(velocity, height, coupling):
    pressure = jnp.einsum("lk,mkc->mlc", coupling, height, precision=lax.Precision.HIGHEST)
    inner = velocity[..., 1:-1]
    moved = inner - time_step * (inner * centred(velocity) + centred(pressure))
    fluxes = moved * height[..., 1:-1]
    height_new = height[..., 2:-2] - time_step * centred(fluxes)
    return (moved[..., 1:-1], height_new)


def advance(members, coupling):
    extended = with_halo(members, "hor", 2 * SUBSTEPS)
    velocity, height = (extended[:, 0], extended[:, 1])
    for step_index in range(SUBSTEPS):
        velocity, height = substep(velocity, height, coupling)
    return velocity, height


def to_slabs(field, slab_count):
    block, levels, cells = field.shape
    return field.reshape(block, slab_count, -1).transpose(1, 0, 2)


def split(value):
    high = value.astype(jnp.bfloat16)
    return high, (value - high.astype(jnp.float32)).astype(jnp.bfloat16)


def product(left, right, across=0):
    dims = (((1,), (across,)), ((), ()))

    def one(a, b):
        return lax.dot_general(a, b, dims, preferred_element_type=jnp.float32)

    left_high, left_low = split(left)
    right_high, right_low = split(right)
    return one(left_high, right_high) + (one(left_high, right_low) + one(left_low, right_high))


def analysis(
    sizes, count,
    seen_ref, value_ref, error_ref, live_ref, blend_ref, height_ref, velocity_ref, out_ref,
    own, column, partial, arrived, peers_blend, gathered, updated, returned,
    send_a, recv_a, send_b, recv_b, send_c, recv_c, send_d, recv_d, send_e, recv_e,
):
    mem_count, grp_count = sizes
    mem = lax.axis_index("mem")
    grp = lax.axis_index("grp")

    def mem_peer(step):
        return lax.rem(mem + step, mem_count)

    def grp_peer(step):
        return lax.rem(grp + step, grp_count)

    barrier = pltpu.get_barrier_semaphore()
    slab = mem * grp_count + grp
    peers = []
    for mem_step in range(mem_count):
        for grp_step in range(grp_count):
            if mem_step + grp_step > 0:
                peers.append((mem_peer(mem_step), grp_peer(grp_step)))
    for one, other in peers:
        pl.semaphore_signal(
            barrier, inc=1, device_id={"mem": one, "grp": other}, device_id_type=MESH
        )

    def exchange(source, target, send_sem, recv_sem):
        copies = []
        for at, (one, other) in enumerate(peers):
            copy = pltpu.make_async_remote_copy(
                src_ref=source.at[one * grp_count + other], dst_ref=target.at[slab],
                send_sem=send_sem.at[at], recv_sem=recv_sem.at[at],
                device_id={"mem": one, "grp": other}, device_id_type=MESH,
            )
            copy.start()
            copies.append(copy)
        return copies


    width = seen_ref.shape[0]
    seen = seen_ref[...]
    average = jnp.mean(seen, axis=0, keepdims=True)
    anomalies = seen - average
    weight = live_ref[...].astype(jnp.float32) / error_ref[...]
    pull = weight * (value_ref[...] - average)
    rows = jnp.concatenate(
        [anomalies * weight, jnp.broadcast_to(pull, (8, pull.shape[1]))], axis=0
    )
    own[...] = product(rows, anomalies, 1)

    pl.semaphore_wait(barrier, mem_count * grp_count - 1)
    blends = []
    for step in range(1, grp_count):
        copy = pltpu.make_async_remote_copy(
            src_ref=blend_ref, dst_ref=peers_blend.at[step - 1],
            send_sem=send_b.at[step - 1], recv_sem=recv_b.at[step - 1],
            device_id={"grp": grp_peer(step)}, device_id_type=MESH,
        )
        copy.start()
        blends.append(copy)
    gathers = []
    for step in range(1, mem_count):
        copy = pltpu.make_async_remote_copy(
            src_ref=own, dst_ref=column.at[step - 1],
            send_sem=send_a.at[step - 1], recv_sem=recv_a.at[step - 1],
            device_id={"mem": mem_peer(step)}, device_id_type=MESH,
        )
        copy.start()
        gathers.append(copy)
    for copy in blends:
        copy.wait()
    lanes = lax.broadcasted_iota(jnp.int32, (1, blend_ref.shape[1]), 1)

    def share(row, step):
        place = lax.rem(mem + mem_count - step, mem_count) * grp_count + grp
        return jnp.sum(jnp.where(lanes == place, row[0:1], 0.0), axis=1, keepdims=True)

    for copy in gathers:
        copy.wait()

    def blended_for(row):
        total = share(row, 0) * own[...]
        for step in range(1, mem_count):
            total = total + share(row, step) * column[step - 1]
        return total

    returns = []
    for step in range(1, grp_count):
        partial[step - 1] = blended_for(peers_blend[step - 1])
        copy = pltpu.make_async_remote_copy(
            src_ref=partial.at[step - 1], dst_ref=arrived.at[step - 1],
            send_sem=send_c.at[step - 1], recv_sem=recv_c.at[step - 1],
            device_id={"grp": grp_peer(grp_count - step)}, device_id_type=MESH,
        )
        copy.start()
        returns.append(copy)
    total = blended_for(blend_ref[...])
    outward = exchange(velocity_ref, gathered, send_d, recv_d)
    gathered[slab] = velocity_ref[slab]
    for copy in returns:
        copy.wait()
    for step in range(1, grp_count):
        total = total + arrived[step - 1]

    total = total / (count + 1.0)
    square = (width, width)
    identity = (
        lax.broadcasted_iota(jnp.int32, square, 0) == lax.broadcasted_iota(jnp.int32, square, 1)
    ).astype(jnp.float32)
    blended = (width - 1.0) * identity + total[:width]
    bvector = total[width:]
    squares = jnp.sum(jnp.sum(blended * blended, axis=1, keepdims=True), axis=0, keepdims=True)
    frobenius = jnp.sqrt(squares)
    iterate = blended / frobenius
    newton = 1.5 * identity - 0.5 * iterate
    inverse_root = newton
    for step in range(1, ROOT_STEPS):
        iterate = product(newton, iterate)
        newton = 1.5 * identity - 0.5 * product(inverse_root, iterate)
        inverse_root = product(newton, inverse_root)
    spread = inverse_root * (jnp.sqrt(width - 1.0) / jnp.sqrt(frobenius))
    inner = product(bvector, inverse_root)
    mean_weight = product(inner, inverse_root) / frobenius
    transposed = spread + mean_weight[0:1]

    def update(flat, field):
        flat_average = jnp.mean(flat, axis=0, keepdims=True)
        result = flat_average + product(transposed, flat - flat_average)
        updated[field] = result.reshape(updated.shape[1:])
        copies = exchange(updated.at[field], returned.at[field], send_e.at[field], recv_e.at[field])
        returned[field, slab] = updated[field, slab]
        return copies

    back = update(height_ref[...], 1)
    for copy in outward:
        copy.wait()
    back = back + update(gathered[...].reshape(height_ref.shape), 0)
    for copy in back:
        copy.wait()
    out_ref[...] = returned[...]


def analysed(sizes, count, seen, value, error, live, blend, height, velocity):
    width = seen.shape[0]
    mem_count, grp_count = sizes
    tall = (width + 8, width)
    vmem = pl.BlockSpec(memory_space=pltpu.VMEM)
    dma = pltpu.SemaphoreType.DMA
    return pl.pallas_call(
        functools.partial(analysis, sizes, count),
        out_shape=jax.ShapeDtypeStruct((2,) + velocity.shape, jnp.float32),
        in_specs=[vmem] * 7,
        out_specs=vmem,
        scratch_shapes=[
            pltpu.VMEM(tall, jnp.float32),
            pltpu.VMEM((mem_count - 1,) + tall, jnp.float32),
            pltpu.VMEM((grp_count - 1,) + tall, jnp.float32),
            pltpu.VMEM((grp_count - 1,) + tall, jnp.float32),
            pltpu.VMEM((grp_count - 1,) + blend.shape, jnp.float32),
            pltpu.VMEM(velocity.shape, jnp.float32),
            pltpu.VMEM((2,) + velocity.shape, jnp.float32),
            pltpu.VMEM((2,) + velocity.shape, jnp.float32),
            dma((mem_count - 1,)), dma((mem_count - 1,)),
            dma((grp_count - 1,)), dma((grp_count - 1,)),
            dma((grp_count - 1,)), dma((grp_count - 1,)),
            dma((mem_count * grp_count - 1,)), dma((mem_count * grp_count - 1,)),
            dma((2, mem_count * grp_count - 1)), dma((2, mem_count * grp_count - 1)),
        ],
        compiler_params=pltpu.CompilerParams(collective_id=0, has_side_effects=True),
    )(seen, value[None], error[None], live[None], blend, height, velocity)


def shards(ensemble, coupling, obs_column, obs_level, obs_value, obs_error, obs_live, partners):
    mem_count = lax.axis_size("mem")
    grp_count = lax.axis_size("grp")
    slab_count = mem_count * grp_count
    own_slab = lax.axis_index("mem") * grp_count + lax.axis_index("grp")
    lanes = max(128, -(-slab_count // 128) * 128)
    slab_numbers = jnp.arange(lanes, dtype=jnp.int32)
    chosen = partners[0, 0]
    count = chosen.shape[0]
    blend_weights = (slab_numbers == own_slab).astype(jnp.float32)
    blend_weights = blend_weights + jnp.sum(
        (slab_numbers[:, None] == chosen[None, :]).astype(jnp.float32), axis=1
    )
    blend = jnp.broadcast_to(blend_weights, (8, lanes))
    width = ensemble.shape[0] * slab_count
    cells = ensemble.shape[3]
    members = ensemble
    for cycle_index in range(obs_column.shape[0]):
        velocity, height = advance(members, coupling)
        heights = lax.all_to_all(
            to_slabs(height, slab_count), ("mem", "grp"), split_axis=0, concat_axis=0, tiled=True
        ).reshape(width, -1)
        place = obs_level[cycle_index, 0, 0] * cells + obs_column[cycle_index, 0, 0]
        observed = jnp.take(heights, place, axis=1)
        result = analysed(
            (mem_count, grp_count), count, observed,
            obs_value[cycle_index, 0, 0], obs_error[cycle_index, 0, 0],
            obs_live[cycle_index, 0, 0], blend, heights, to_slabs(velocity, slab_count),
        )
        shaped = result.reshape(2, slab_count, ensemble.shape[0], -1, cells)
        members = shaped.transpose(2, 0, 1, 3, 4).reshape(ensemble.shape)
    return members


def solution(mesh):
    in_specs = (
        P(("mem", "grp"), None, None, "hor"),
        P(),
        P(None, ("mem", "grp"), "hor", None),
        P(None, ("mem", "grp"), "hor", None),
        P(None, ("mem", "grp"), "hor", None),
        P(None, ("mem", "grp"), "hor", None),
        P(None, ("mem", "grp"), "hor", None),
        P(("mem", "grp"), "hor", None),
    )
    out_specs = P(("mem", "grp"), None, None, "hor")
    return jax.shard_map(shards, mesh=mesh, in_specs=in_specs, out_specs=out_specs, check_vma=False)
```
